8 devices in a mesh: dp: 1 (over z), col: 2 (over y), row: 4 (over x, core).
Axes of the slice: x: 2, y: 2, z: 1, core: 2. Of those that a mesh axis runs over, the one named last changes fastest.
Arguments:
- x_act: bfloat16 [96, 8192], P(('dp', 'row'), 'col')
- ln_gain: float32 [8192], P('col')
- w_in: bfloat16 [8192, 32768], P('row', 'col')
- w_out: bfloat16 [32768, 8192], P('row', 'col')
Outputs:
- output: bfloat16 [96, 8192], P(('dp', 'row'), 'col')
All inputs are finite; a program needn't handle non-finite values.
Results may differ from the reference program's by a relative error of at most 0.00135.
Values are sent between devices in bfloat16 or wider.
A program may use at most 1 GiB of HBM per device.

```python
import jax
import jax.numpy as jnp
from jax import lax

TOKENS = 96
D_MODEL = 8192
D_FF = 32768

NORM_EPS = 1e-5


def setup_inputs(seed: int = 0, part: int = 0) -> dict:
    key = jax.random.key(seed)
    part_key, shared_key = jax.random.split(key)
    part_key = jax.random.fold_in(part_key, part)
    key_noise, key_row, key_shift, key_scale = jax.random.split(part_key, 4)
    key_gain, key_in, key_out = jax.random.split(shared_key, 3)
    walk_norm = D_MODEL ** -0.5
    feat_shift = 0.8 * walk_norm * jnp.cumsum(jax.random.normal(key_shift, (D_MODEL,), jnp.float32))
    feat_scale = jnp.exp(0.5 * walk_norm * jnp.cumsum(jax.random.normal(key_scale, (D_MODEL,), jnp.float32)))
    row_shift = 0.5 * jax.random.normal(key_row, (TOKENS, 1), jnp.float32)
    noise = jax.random.normal(key_noise, (TOKENS, D_MODEL), jnp.float32)
    x_act = (noise * feat_scale + feat_shift + row_shift).astype(jnp.bfloat16)
    ln_gain = jax.random.uniform(key_gain, (D_MODEL,), jnp.float32, 0.5, 1.5)
    w_in = (D_MODEL ** -0.5 * jax.random.normal(key_in, (D_MODEL, D_FF), jnp.float32)).astype(jnp.bfloat16)
    w_out = (1.5 * D_FF ** -0.5 * jax.random.normal(key_out, (D_FF, D_MODEL), jnp.float32)).astype(jnp.bfloat16)
    return {"x_act": x_act, "ln_gain": ln_gain, "w_in": w_in, "w_out": w_out}


def reference(x_act, ln_gain, w_in, w_out):
    x_f32 = x_act.astype(jnp.float32)
    row_mean = jnp.mean(x_f32, axis=1, keepdims=True)
    row_var = jnp.mean(x_f32 * x_f32, axis=1, keepdims=True) - row_mean * row_mean
    z_norm = ((x_f32 - row_mean) * lax.rsqrt(row_var + NORM_EPS) * ln_gain).astype(jnp.bfloat16)
    hidden = jax.nn.gelu(jnp.dot(z_norm, w_in, preferred_element_type=jnp.float32), approximate=True).astype(jnp.bfloat16)
    branch = jnp.dot(hidden, w_out, preferred_element_type=jnp.float32)
    return (x_f32 + branch).astype(jnp.bfloat16)
```

```python
import functools
import math

import jax
import jax.numpy as jnp
from jax import lax
from jax.experimental import pallas as pl
from jax.experimental.pallas import tpu as pltpu
from jax.sharding import PartitionSpec as P

NORM_EPS = 1e-5
MESH = pl.DeviceIdType.MESH

TOK = 24
ROWS = 4
T = 16
NB = 32
NA = 40
ND = 24
NU = 5
NDN = 5
LA, LB, LG, LF, LD = 2, 4, 6, 8, 10
FC = 4


def gelu_tanh(v):
    inner = math.sqrt(2.0 / math.pi) * (v + 0.044715 * (v * v * v))
    return v * (0.5 * (1.0 + jnp.tanh(inner)))


def mlp_kernel(
    x_hbm, g_hbm, wi_hbm, wo_hbm, y_ref,
    xv, gv, xblk, gblk, stat, z, usl, dsl, p_own, p_oth, r_d2d, xr, t1, t2, t3, h, hs, acc, dr, fs, xr2,
    ld_s, xs_s, xs_r, g_s, g_r, st_s, st_r, u_sem, d_sem,
    d2d_s, d2d_r, xa_s, xa_r, xb_s, xb_r, t1_s, t1_r, t2_s, t2_r, t3_s, t3_r,
    hb_s, hb_r, hay_s, hay_r, hby_s, hby_r, f_s, f_r, f2_s, f2_r,
):
    r = lax.axis_index("row")
    c = lax.axis_index("col")
    xc = r // 2
    q = r % 2
    home = xc == c
    peer = xc != c
    pair = 2 * xc + (1 - q)
    xrow = 2 * (1 - xc) + q
    ycol = 1 - c
    d_loc = x_hbm.shape[1]
    kdim = z.shape[1]
    w = h.shape[2]
    ntok = ROWS * TOK
    d_model = 2 * d_loc
    half = T * w

    def rcopy(src, dst, ssem, rsem, row, col):
        return pltpu.make_async_remote_copy(
            src_ref=src, dst_ref=dst, send_sem=ssem, recv_sem=rsem,
            device_id={"row": row, "col": col}, device_id_type=MESH)

    ld_x = pltpu.make_async_copy(x_hbm, xv, ld_s.at[0])
    ld_g = pltpu.make_async_copy(g_hbm, gv, ld_s.at[1])
    ld_x.start()
    ld_g.start()

    def u_copy(s, k):
        slot = lax.rem(s, NU)
        side = q if k == 1 else 1 - q
        cols = pl.ds(pl.multiple_of(side * half + s * w, w), w)
        return pltpu.make_async_copy(wi_hbm.at[:, cols], usl.at[slot, k], u_sem.at[slot, k])

    def d_copy(s):
        slot = lax.rem(s, NDN)
        rows = pl.ds(pl.multiple_of(s * w, w), w)
        return pltpu.make_async_copy(wo_hbm.at[rows, :], dsl.at[slot], d_sem.at[slot])

    for s in range(NU):
        u_copy(s, 0).start()
        u_copy(s, 1).start()
    for s in range(NDN):
        d_copy(s).start()

    barrier = pltpu.get_barrier_semaphore()
    for k in range(1, 2 * ROWS):
        rr = lax.rem(r + k, ROWS)
        cc = lax.rem(c + k // ROWS, 2)
        pl.semaphore_signal(barrier, inc=1, device_id={"row": rr, "col": cc}, device_id_type=MESH)
    pl.semaphore_wait(barrier, 2 * ROWS - 1)

    ld_x.wait()

    def x_copy(j, k):
        return rcopy(xv.at[:, pl.ds(j * kdim, kdim)], xblk.at[r], xs_s.at[j, k], xs_r.at[r],
                     2 * c + j, c if k == 0 else ycol)

    for k in (1, 0):
        for j in range(2):
            if k == 1:
                x_copy(j, k).start()
            else:
                @pl.when(2 * c + j != r)
                def _():
                    x_copy(j, k).start()

                @pl.when(2 * c + j == r)
                def _():
                    xblk[2 * c + j] = xv[:, j * kdim:(j + 1) * kdim]

    ld_g.wait()

    def g_copy():
        return rcopy(gv.at[:, pl.ds(pl.multiple_of(q * kdim, kdim), kdim)], gblk, g_s, g_r, r, ycol)

    @pl.when(home)
    def _():
        g_copy().start()
        gblk[...] = gv[:, pl.ds(pl.multiple_of(q * kdim, kdim), kdim)]

    s1 = jnp.zeros((TOK, 128), jnp.float32)
    s2 = jnp.zeros((TOK, 128), jnp.float32)
    for j in range(d_loc // 128):
        v = xv[:, j * 128:(j + 1) * 128].astype(jnp.float32)
        s1 = s1 + v
        s2 = s2 + v * v
    s1 = jnp.sum(s1, axis=1, keepdims=True)
    s2 = jnp.sum(s2, axis=1, keepdims=True)
    lane = lax.broadcasted_iota(jnp.int32, (TOK, 128), 1)
    me = c * ROWS + r
    stat[me] = jnp.where(lane == 0, s1, s2)

    acc[...] = jnp.zeros_like(acc)

    def st_copy(k):
        rr = lax.rem(r + k, ROWS)
        cc = lax.rem(c + k // ROWS, 2)
        return rcopy(stat.at[me], stat.at[me], st_s.at[k], st_r.at[me], rr, cc)

    for k in range(1, 2 * ROWS):
        st_copy(k).start()

    for k in range(1, 2 * ROWS):
        src = lax.rem(c + k // ROWS, 2) * ROWS + lax.rem(r + k, ROWS)
        rcopy(stat.at[src], stat.at[src], st_s.at[k], st_r.at[src], r, ycol).wait_recv()
    for rr in range(ROWS):
        @pl.when(jnp.logical_or(r != rr, peer))
        def _():
            rcopy(xblk.at[rr], xblk.at[rr], xs_s.at[0, 0], xs_r.at[rr], r, ycol).wait_recv()

    @pl.when(peer)
    def _():
        g_copy().wait_recv()

    means, invs = [], []
    for rr in range(ROWS):
        tot = stat[rr] + stat[ROWS + rr]
        mean = tot[:, 0:1] / d_model
        var = tot[:, 1:2] / d_model - mean * mean
        means.append(mean)
        invs.append(lax.rsqrt(var + NORM_EPS))
    zw = 512
    for j in range(kdim // zw):
        cols = slice(j * zw, (j + 1) * zw)
        g = gblk[:, cols]
        parts = []
        for rr in range(ROWS):
            v = xblk[rr, :, cols].astype(jnp.float32)
            parts.append((v - means[rr]) * invs[rr] * g)
        z[:, cols] = jnp.concatenate(parts, axis=0).astype(jnp.bfloat16)

    def d2d(u):
        return rcopy(p_oth.at[u], r_d2d.at[u], d2d_s.at[u], d2d_r.at[u], pair, c)

    def xa(u):
        return rcopy(p_own.at[u, pl.ds(NB, NA)], xr.at[u, pl.ds(0, NA)], xa_s.at[u], xa_r.at[u], xrow, c)

    def xb(u):
        return rcopy(p_own.at[u, pl.ds(0, NB)], xr.at[u, pl.ds(0, NB)], xb_s.at[u], xb_r.at[u], xrow, c)

    def tr1(u):
        return rcopy(p_own.at[u, pl.ds(NB + NA, ND)], t1.at[u], t1_s.at[u], t1_r.at[u], r, ycol)

    def tr2(u):
        return rcopy(t1.at[u], t2.at[u], t2_s.at[u], t2_r.at[u], xrow, c)

    def tr3(u):
        return rcopy(t2.at[u], t3.at[u], t3_s.at[u], t3_r.at[u], r, ycol)

    def hb(u):
        return rcopy(hs.at[u], h.at[u, pl.ds(0, NB)], hb_s.at[u], hb_r.at[u], xrow, c)

    def hay(u):
        rows = pl.ds(NB, ntok - NB)
        return rcopy(h.at[u, rows], h.at[u, rows], hay_s.at[u], hay_r.at[u], r, ycol)

    def hby(u):
        rows = pl.ds(0, NB)
        return rcopy(h.at[u, rows], h.at[u, rows], hby_s.at[u], hby_r.at[u], r, ycol)

    def live(v):
        return jnp.logical_and(v >= 0, v < T)

    def step(s, carry):
        if ND:
            va = s - LA

            @pl.when(jnp.logical_and(live(va), home))
            def _():
                tr1(va).wait_recv()
                tr2(va).start()

            vb = s - LB

            @pl.when(jnp.logical_and(live(vb), peer))
            def _():
                tr2(vb).wait_recv()
                tr3(vb).start()

        vg = s - LG

        @pl.when(jnp.logical_and(live(vg), home))
        def _():
            xa(vg).wait_recv()
            got = xr[vg, 0:NA]
            if ND:
                tr3(vg).wait_recv()
                got = jnp.concatenate([got, t3[vg]], axis=0)
            h[vg, NB:ntok] = gelu_tanh(p_own[vg, NB:ntok] + got).astype(jnp.bfloat16)

        @pl.when(jnp.logical_and(live(vg), peer))
        def _():
            xb(vg).wait_recv()
            hs[vg] = gelu_tanh(p_own[vg, 0:NB] + xr[vg, 0:NB]).astype(jnp.bfloat16)

        slot = lax.rem(s, NU)

        @pl.when(s < T)
        def _():
            u_copy(s, 0).wait()
            p_oth[s] = jnp.dot(z[...], usl[slot, 0], preferred_element_type=jnp.float32)

        @pl.when(jnp.logical_and(live(vg), home))
        def _():
            hay(vg).start()

        @pl.when(jnp.logical_and(live(vg), peer))
        def _():
            hb(vg).start()

        u = s - 1

        @pl.when(live(u))
        def _():
            d2d(u).wait_recv()
            p_own[u] = p_own[u] + r_d2d[u]

        @pl.when(s < T)
        def _():
            d2d(s).start()

        @pl.when(jnp.logical_and(live(u), home))
        def _():
            xb(u).start()

        @pl.when(jnp.logical_and(live(u), peer))
        def _():
            if ND:
                tr1(u).start()
            xa(u).start()

        @pl.when(s < T)
        def _():
            u_copy(s, 1).wait()
            p_own[s] = jnp.dot(z[...], usl[slot, 1], preferred_element_type=jnp.float32)

        @pl.when(s + NU < T)
        def _():
            u_copy(s + NU, 0).start()
            u_copy(s + NU, 1).start()

        vf = s - LF

        @pl.when(jnp.logical_and(live(vf), home))
        def _():
            hb(vf).wait_recv()
            hby(vf).start()

        vd = s - LD

        @pl.when(live(vd))
        def _():
            @pl.when(peer)
            def _():
                hay(vd).wait_recv()
                hby(vd).wait_recv()

            d_copy(vd).wait()
            dslot = lax.rem(vd, NDN)
            hv = h[vd]
            nw = 512
            for n in range(d_loc // nw):
                cols = slice(n * nw, (n + 1) * nw)
                out = jnp.dot(hv, dsl[dslot, :, cols], preferred_element_type=jnp.float32)
                acc[:, :, cols] = acc[:, :, cols] + out.reshape(ROWS, TOK, nw)

            @pl.when(vd + NDN < T)
            def _():
                d_copy(vd + NDN).start()

        return carry

    lax.fori_loop(0, T + LD, step, 0)

    fw = d_loc // FC
    mine_far = 2 * (1 - xc) + q
    pair_far = 2 * (1 - xc) + (1 - q)

    def fcols(k):
        return pl.ds(k * fw, fw)

    def f_copy(i, k):
        tok = pair_far if i == 0 else pair
        return rcopy(acc.at[tok, :, fcols(k)], dr.at[i, :, fcols(k)], f_s.at[i, k], f_r.at[i, k], pair, c)

    def f2_copy(k):
        return rcopy(fs.at[:, fcols(k)], xr2.at[:, fcols(k)], f2_s.at[k], f2_r.at[k], xrow, c)

    for i in range(2):
        for k in range(FC):
            f_copy(i, k).start()
    for k in range(FC):
        cols = slice(k * fw, (k + 1) * fw)
        f_copy(0, k).wait_recv()
        fs[:, cols] = acc[mine_far, :, cols] + dr[0, :, cols]
        if k:
            f2_copy(k - 1).start()
    for k in range(FC):
        cols = slice(k * fw, (k + 1) * fw)
        f_copy(1, k).wait_recv()
        acc[r, :, cols] = acc[r, :, cols] + dr[1, :, cols]
        if k == 0:
            f2_copy(FC - 1).start()

    for k in (1, 0):
        for j in range(2):
            if k == 1:
                x_copy(j, k).wait_send()
            else:
                @pl.when(2 * c + j != r)
                def _():
                    x_copy(j, k).wait_send()

    @pl.when(home)
    def _():
        g_copy().wait_send()

    for k in range(1, 2 * ROWS):
        st_copy(k).wait_send()

    def drain(u, carry):
        d2d(u).wait_send()

        @pl.when(home)
        def _():
            xb(u).wait_send()
            if ND:
                tr2(u).wait_send()
            hay(u).wait_send()
            hby(u).wait_send()

        @pl.when(peer)
        def _():
            xa(u).wait_send()
            if ND:
                tr1(u).wait_send()
                tr3(u).wait_send()
            hb(u).wait_send()

        return carry

    lax.fori_loop(0, T, drain, 0)

    for k in range(FC):
        cols = slice(k * fw, (k + 1) * fw)
        f2_copy(k).wait_recv()
        branch = acc[r, :, cols] + xr2[:, cols]
        y_ref[:, cols] = (xv[:, cols].astype(jnp.float32) + branch).astype(jnp.bfloat16)
    for k in range(FC):
        for i in range(2):
            f_copy(i, k).wait_send()
        f2_copy(k).wait_send()


def solution(mesh):
    def local_block(x_blk, gain_blk, w_in_blk, w_out_blk):
        d_loc = x_blk.shape[1]
        kdim, ff_loc = w_in_blk.shape
        w = ff_loc // (2 * T)
        ntok = ROWS * TOK
        f32, bf16 = jnp.float32, jnp.bfloat16
        dma = pltpu.SemaphoreType.DMA
        nd = max(ND, 8)
        scratch = [
            pltpu.VMEM((TOK, d_loc), bf16),
            pltpu.VMEM((1, d_loc), f32),
            pltpu.VMEM((ROWS, TOK, kdim), bf16),
            pltpu.VMEM((1, kdim), f32),
            pltpu.VMEM((2 * ROWS, TOK, 128), f32),
            pltpu.VMEM((ntok, kdim), bf16),
            pltpu.VMEM((NU, 2, kdim, w), bf16),
            pltpu.VMEM((NDN, w, d_loc), bf16),
            pltpu.VMEM((T, ntok, w), f32),
            pltpu.VMEM((T, ntok, w), f32),
            pltpu.VMEM((T, ntok, w), f32),
            pltpu.VMEM((T, max(NA, NB), w), f32),
            pltpu.VMEM((T, nd, w), f32),
            pltpu.VMEM((T, nd, w), f32),
            pltpu.VMEM((T, nd, w), f32),
            pltpu.VMEM((T, ntok, w), bf16),
            pltpu.VMEM((T, NB, w), bf16),
            pltpu.VMEM((ROWS, TOK, d_loc), f32),
            pltpu.VMEM((2, TOK, d_loc), f32),
            pltpu.VMEM((TOK, d_loc), f32),
            pltpu.VMEM((TOK, d_loc), f32),
            dma((2,)), dma((2, 2)), dma((ROWS,)), dma, dma, dma((2 * ROWS,)), dma((2 * ROWS,)),
            dma((NU, 2)), dma((NDN,)),
        ] + [dma((T,))] * 18 + [dma((2, FC)), dma((2, FC)), dma((FC,)), dma((FC,))]
        return pl.pallas_call(
            mlp_kernel,
            out_shape=jax.ShapeDtypeStruct((TOK, d_loc), bf16),
            in_specs=[pl.BlockSpec(memory_space=pl.ANY)] * 4,
            out_specs=pl.BlockSpec(memory_space=pltpu.VMEM),
            scratch_shapes=scratch,
            compiler_params=pltpu.CompilerParams(
                collective_id=0, has_side_effects=True, vmem_limit_bytes=67_043_328),
        )(x_blk, gain_blk.reshape(1, d_loc), w_in_blk, w_out_blk)

    return jax.shard_map(
        local_block,
        mesh=mesh,
        in_specs=(P(("dp", "row"), "col"), P("col"), P("row", "col"), P("row", "col")),
        out_specs=P(("dp", "row"), "col"),
        check_vma=False,
    )
```

```python
import functools
import math

import jax
import jax.numpy as jnp
from jax import lax
from jax.experimental import pallas as pl
from jax.experimental.pallas import tpu as pltpu
from jax.sharding import PartitionSpec as P

NORM_EPS = 1e-5
MESH = pl.DeviceIdType.MESH

TOK = 24
ROWS = 4
T = 16
NB = 32
NA = 40
ND = 24
NU = 5
NDN = 5
XRELAY = 3
LA, LB, LG, LF = 3, 5, 7, 8
LH, LP = 8, 10
LX = 3
TN = T - 1
NP = 3
FC = 4


def gelu_tanh(v):
    inner = math.sqrt(2.0 / math.pi) * (v + 0.044715 * (v * v * v))
    return v * (0.5 * (1.0 + jnp.tanh(inner)))


def mlp_kernel(
    x_hbm, g_hbm, wi_hbm, wo_hbm, y_ref,
    xv, gv, xblk, xrel, gblk, stat, z, usl, dsl, p_own, p_oth, r_d2d, xr, xl, t1, t2, t3, h, hs, acc, dr, fs, xr2,
    ld_s, xs_s, xs_r, xo_s, xo_r, xl_s, xl_r, hl_s, hl_r, g_s, g_r, st_s, st_r, u_sem, d_sem,
    d2d_s, d2d_r, xa_s, xa_r, xb_s, xb_r, t1_s, t1_r, t2_s, t2_r, t3_s, t3_r,
    hb_s, hb_r, hay_s, hay_r, hby_s, hby_r, f_s, f_r, f2_s, f2_r,
):
    r = lax.axis_index("row")
    c = lax.axis_index("col")
    xc = r // 2
    q = r % 2
    home = xc == c
    peer = xc != c
    pair = 2 * xc + (1 - q)
    xrow = 2 * (1 - xc) + q
    ycol = 1 - c
    d_loc = x_hbm.shape[1]
    kdim = z.shape[1]
    w = h.shape[2]
    ntok = ROWS * TOK
    d_model = 2 * d_loc
    half = T * w

    def rcopy(src, dst, ssem, rsem, row, col):
        return pltpu.make_async_remote_copy(
            src_ref=src, dst_ref=dst, send_sem=ssem, recv_sem=rsem,
            device_id={"row": row, "col": col}, device_id_type=MESH)

    ld_x = pltpu.make_async_copy(x_hbm, xv, ld_s.at[0])
    ld_g = pltpu.make_async_copy(g_hbm, gv, ld_s.at[1])
    ld_x.start()
    ld_g.start()

    barrier = pltpu.get_barrier_semaphore()
    for k in range(1, 2 * ROWS):
        rr = lax.rem(r + k, ROWS)
        cc = lax.rem(c + k // ROWS, 2)
        pl.semaphore_signal(barrier, inc=1, device_id={"row": rr, "col": cc}, device_id_type=MESH)

    def u_copy(s, k):
        slot = lax.rem(s, NU)
        side = q if k == 1 else 1 - q
        cols = pl.ds(pl.multiple_of(side * half + s * w, w), w)
        return pltpu.make_async_copy(wi_hbm.at[:, cols], usl.at[slot, k], u_sem.at[slot, k])

    def d_copy(s):
        slot = lax.rem(s, NDN)
        rows = pl.ds(pl.multiple_of(s * w, w), w)
        return pltpu.make_async_copy(wo_hbm.at[rows, :], dsl.at[slot], d_sem.at[slot])

    ld_x.wait()
    ld_g.wait()
    for s in range(NU):
        u_copy(s, 0).start()
        u_copy(s, 1).start()
    for s in range(NDN):
        d_copy(s).start()

    s1 = jnp.zeros((TOK, 128), jnp.float32)
    s2 = jnp.zeros((TOK, 128), jnp.float32)
    for j in range(d_loc // 128):
        v = xv[:, j * 128:(j + 1) * 128].astype(jnp.float32)
        s1 = s1 + v
        s2 = s2 + v * v
    s1 = jnp.sum(s1, axis=1, keepdims=True)
    s2 = jnp.sum(s2, axis=1, keepdims=True)
    lane = lax.broadcasted_iota(jnp.int32, (8, 128), 1)
    me = c * ROWS + r
    st = jnp.zeros((8, 128), jnp.float32)
    for i in range(TOK // 8):
        st = jnp.where(lane == 2 * i, s1[8 * i:8 * i + 8], st)
        st = jnp.where(lane == 2 * i + 1, s2[8 * i:8 * i + 8], st)
    stat[me] = st

    @pl.when(home)
    def _():
        gblk[...] = gv[:, pl.ds(pl.multiple_of(q * kdim, kdim), kdim)]
        for j in range(2):
            @pl.when(q == j)
            def _():
                xblk[r] = xv[:, j * kdim:(j + 1) * kdim]

    pl.semaphore_wait(barrier, 2 * ROWS - 1)

    def st_copy(k):
        rr = lax.rem(r + k, ROWS)
        cc = lax.rem(c + k // ROWS, 2)
        return rcopy(stat.at[me], stat.at[me], st_s.at[k], st_r.at[me], rr, cc)

    for k in range(1, 2 * ROWS):
        st_copy(k).start()

    xw = kdim // 2

    def xcols(j, p):
        return pl.ds(j * kdim + p * xw, xw)

    def xs_home_pair(p):
        cols = pl.ds(pl.multiple_of((1 - q) * kdim + p * xw, xw), xw)
        return rcopy(xv.at[:, cols], xblk.at[r, :, pl.ds(p * xw, xw)], xs_s.at[0, p], xs_r.at[r, p], pair, c)

    def xs_home_y(j, p):
        return rcopy(xv.at[:, xcols(j, p)], xblk.at[r, :, pl.ds(p * xw, xw)], xs_s.at[1 + j, p], xs_r.at[r, p],
                     2 * xc + j, ycol)

    def xs_peer_x(j, p):
        return rcopy(xv.at[:, xcols(j, p)], xblk.at[r, :, pl.ds(p * xw, xw)], xs_s.at[j, p], xs_r.at[r, p],
                     2 * (1 - xc) + j, c)

    def xs_peer_far(j, p):
        return rcopy(xv.at[:, xcols(j, p)], xblk.at[r, :, pl.ds(p * xw, xw)], xs_s.at[2 + j, p], xs_r.at[r, p],
                     2 * (1 - xc) + j, ycol)

    def xs_relay_in(j, p):
        return rcopy(xv.at[:, xcols(j, p)], xrel.at[j, p], xs_s.at[2 + j, p], xo_r.at[j, p], r, ycol)

    def xs_relay_out(j, p):
        return rcopy(xrel.at[j, p], xblk.at[r, :, pl.ds(p * xw, xw)], xo_s.at[j, p], xs_r.at[r, p],
                     2 * (1 - xc) + j, c)

    pieces = [(j, p) for p in range(2) for j in range(2)]

    def g_copy():
        return rcopy(gv.at[:, pl.ds(pl.multiple_of(q * kdim, kdim), kdim)], gblk, g_s, g_r, r, ycol)

    @pl.when(home)
    def _():
        for j, p in pieces:
            xs_home_y(j, p).start()
        for p in range(2):
            xs_home_pair(p).start()
        g_copy().start()

    @pl.when(peer)
    def _():
        for n, (j, p) in enumerate(pieces):
            if n < XRELAY:
                xs_relay_in(j, p).start()
            else:
                xs_peer_far(j, p).start()
        for j, p in pieces:
            xs_peer_x(j, p).start()

    acc[...] = jnp.zeros_like(acc)

    @pl.when(home)
    def _():
        for n, (j, p) in enumerate(pieces):
            if n < XRELAY:
                xs_relay_in(j, p).wait_recv()
                xs_relay_out(j, p).start()

    for k in range(1, 2 * ROWS):
        src = lax.rem(c + k // ROWS, 2) * ROWS + lax.rem(r + k, ROWS)
        rcopy(stat.at[src], stat.at[src], st_s.at[k], st_r.at[src], r, ycol).wait_recv()
    for p in range(2):
        for rr in range(ROWS):
            @pl.when(jnp.logical_or(r != rr, peer))
            def _():
                half_blk = xblk.at[rr, :, pl.ds(p * xw, xw)]
                rcopy(half_blk, half_blk, xs_s.at[0, 0], xs_r.at[rr, p], r, ycol).wait_recv()

    @pl.when(peer)
    def _():
        g_copy().wait_recv()

    means, invs = [], []
    for rr in range(ROWS):
        tot = (stat[rr] + stat[ROWS + rr]) / d_model
        mean = jnp.concatenate([tot[:, 2 * i:2 * i + 1] for i in range(TOK // 8)], axis=0)
        var = jnp.concatenate([tot[:, 2 * i + 1:2 * i + 2] for i in range(TOK // 8)], axis=0) - mean * mean
        means.append(mean)
        invs.append(lax.rsqrt(var + NORM_EPS))
    zw = 512
    for j in range(kdim // zw):
        cols = slice(j * zw, (j + 1) * zw)
        g = gblk[:, cols]
        parts = []
        for rr in range(ROWS):
            v = xblk[rr, :, cols].astype(jnp.float32)
            parts.append((v - means[rr]) * invs[rr] * g)
        z[:, cols] = jnp.concatenate(parts, axis=0).astype(jnp.bfloat16)

    def d2d(u):
        return rcopy(p_oth.at[u], r_d2d.at[u], d2d_s.at[u], d2d_r.at[u], pair, c)

    def xa(u):
        return rcopy(p_own.at[u, pl.ds(NB, NA)], xr.at[u, pl.ds(0, NA)], xa_s.at[u], xa_r.at[u], xrow, c)

    prow = ntok // NP

    def xl_copy(i):
        rows = pl.ds(pl.multiple_of(i * prow, prow), prow)
        return rcopy(p_own.at[TN, rows], xl.at[rows], xl_s.at[i], xl_r.at[i], xrow, c)

    def xb(u):
        return rcopy(p_own.at[u, pl.ds(0, NB)], xr.at[u, pl.ds(0, NB)], xb_s.at[u], xb_r.at[u], xrow, c)

    def tr1(u):
        return rcopy(p_own.at[u, pl.ds(NB + NA, ND)], t1.at[u], t1_s.at[u], t1_r.at[u], r, ycol)

    def tr2(u):
        return rcopy(t1.at[u], t2.at[u], t2_s.at[u], t2_r.at[u], xrow, c)

    def tr3(u):
        return rcopy(t2.at[u], t3.at[u], t3_s.at[u], t3_r.at[u], r, ycol)

    def hb(u):
        return rcopy(hs.at[u], h.at[u, pl.ds(0, NB)], hb_s.at[u], hb_r.at[u], xrow, c)

    def hay(u):
        rows = pl.ds(NB, ntok - NB)
        return rcopy(h.at[u, rows], h.at[u, rows], hay_s.at[u], hay_r.at[u], r, ycol)

    def hl_copy(i):
        rows = pl.ds(pl.multiple_of(i * prow, prow), prow)
        return rcopy(h.at[TN, rows], h.at[TN, rows], hl_s.at[i], hl_r.at[i], r, ycol)

    def hby(u):
        rows = pl.ds(0, NB)
        return rcopy(h.at[u, rows], h.at[u, rows], hby_s.at[u], hby_r.at[u], r, ycol)

    def live(v):
        return jnp.logical_and(v >= 0, v < TN)

    def live_piece(i):
        return jnp.logical_and(i >= 0, i < NP)

    def step(s, carry):
        if ND:
            va = s - LA

            @pl.when(jnp.logical_and(live(va), home))
            def _():
                tr1(va).wait_recv()
                tr2(va).start()

            vb = s - LB

            @pl.when(jnp.logical_and(live(vb), peer))
            def _():
                tr2(vb).wait_recv()
                tr3(vb).start()

        vg = s - LG

        @pl.when(jnp.logical_and(live(vg), home))
        def _():
            xa(vg).wait_recv()
            got = xr[vg, 0:NA]
            if ND:
                tr3(vg).wait_recv()
                got = jnp.concatenate([got, t3[vg]], axis=0)
            h[vg, NB:ntok] = gelu_tanh(p_own[vg, NB:ntok] + got).astype(jnp.bfloat16)

        @pl.when(jnp.logical_and(live(vg), peer))
        def _():
            xb(vg).wait_recv()
            hs[vg] = gelu_tanh(p_own[vg, 0:NB] + xr[vg, 0:NB]).astype(jnp.bfloat16)

        ig = s - T - LX

        @pl.when(jnp.logical_and(live_piece(ig), home))
        def _():
            xl_copy(ig).wait_recv()
            rows = pl.ds(pl.multiple_of(ig * prow, prow), prow)
            h[TN, rows] = gelu_tanh(p_own[TN, rows] + xl[rows]).astype(jnp.bfloat16)

        slot = lax.rem(s, NU)

        @pl.when(s < T)
        def _():
            u_copy(s, 0).wait()
            p_oth[s] = jnp.dot(z[...], usl[slot, 0], preferred_element_type=jnp.float32)

        @pl.when(jnp.logical_and(live(vg), home))
        def _():
            hay(vg).start()

        @pl.when(jnp.logical_and(live_piece(ig), home))
        def _():
            hl_copy(ig).start()

        @pl.when(jnp.logical_and(live(vg), peer))
        def _():
            hb(vg).start()

        u = s - 1

        @pl.when(jnp.logical_and(u >= 0, u < T))
        def _():
            d2d(u).wait_recv()
            p_own[u] = p_own[u] + r_d2d[u]

        @pl.when(s < T)
        def _():
            d2d(s).start()

        @pl.when(jnp.logical_and(live(u), home))
        def _():
            xb(u).start()

        @pl.when(jnp.logical_and(live(u), peer))
        def _():
            if ND:
                tr1(u).start()
            xa(u).start()

        @pl.when(jnp.logical_and(live_piece(s - T), peer))
        def _():
            xl_copy(s - T).start()

        @pl.when(s < T)
        def _():
            u_copy(s, 1).wait()
            p_own[s] = jnp.dot(z[...], usl[slot, 1], preferred_element_type=jnp.float32)

        @pl.when(s + NU < T)
        def _():
            u_copy(s + NU, 0).start()
            u_copy(s + NU, 1).start()

        vf = s - LF

        @pl.when(jnp.logical_and(live(vf), home))
        def _():
            hb(vf).wait_recv()
            hby(vf).start()

        vd = s - jnp.where(home, LH, LP)

        @pl.when(jnp.logical_and(vd >= 0, vd < T))
        def _():
            @pl.when(jnp.logical_and(live(vd), peer))
            def _():
                hay(vd).wait_recv()
                hby(vd).wait_recv()

            @pl.when(jnp.logical_and(vd == TN, peer))
            def _():
                for i in range(NP):
                    hl_copy(i).wait_recv()

            d_copy(vd).wait()
            dslot = lax.rem(vd, NDN)
            hv = h[vd]
            nw = 512
            for n in range(d_loc // nw):
                cols = slice(n * nw, (n + 1) * nw)
                out = jnp.dot(hv, dsl[dslot, :, cols], preferred_element_type=jnp.float32)
                acc[:, :, cols] = acc[:, :, cols] + out.reshape(ROWS, TOK, nw)

            @pl.when(vd + NDN < T)
            def _():
                d_copy(vd + NDN).start()

        return carry

    lax.fori_loop(0, T + LP, step, 0)

    fw = d_loc // FC
    mine_far = 2 * (1 - xc) + q
    pair_far = 2 * (1 - xc) + (1 - q)

    def fcols(k):
        return pl.ds(k * fw, fw)

    def f_copy(i, k):
        tok = pair_far if i == 0 else pair
        return rcopy(acc.at[tok, :, fcols(k)], dr.at[i, :, fcols(k)], f_s.at[i, k], f_r.at[i, k], pair, c)

    def f2_copy(k):
        return rcopy(fs.at[:, fcols(k)], xr2.at[:, fcols(k)], f2_s.at[k], f2_r.at[k], xrow, c)

    for i in range(2):
        for k in range(FC):
            f_copy(i, k).start()
    for k in range(FC):
        cols = slice(k * fw, (k + 1) * fw)
        f_copy(0, k).wait_recv()
        fs[:, cols] = acc[mine_far, :, cols] + dr[0, :, cols]
        if k:
            f2_copy(k - 1).start()
    for k in range(FC):
        cols = slice(k * fw, (k + 1) * fw)
        f_copy(1, k).wait_recv()
        acc[r, :, cols] = acc[r, :, cols] + dr[1, :, cols]
        if k == 0:
            f2_copy(FC - 1).start()

    @pl.when(home)
    def _():
        for j, p in pieces:
            xs_home_y(j, p).wait_send()
        for p in range(2):
            xs_home_pair(p).wait_send()
        g_copy().wait_send()
        for j, p in pieces[:XRELAY]:
            xs_relay_out(j, p).wait_send()

    @pl.when(peer)
    def _():
        for j, p in pieces:
            xs_peer_x(j, p).wait_send()
            xs_peer_far(j, p).wait_send()

    for k in range(1, 2 * ROWS):
        st_copy(k).wait_send()

    def drain(u, carry):
        d2d(u).wait_send()

        @pl.when(jnp.logical_and(live(u), home))
        def _():
            xb(u).wait_send()
            if ND:
                tr2(u).wait_send()
            hay(u).wait_send()
            hby(u).wait_send()

        @pl.when(jnp.logical_and(live(u), peer))
        def _():
            xa(u).wait_send()
            if ND:
                tr1(u).wait_send()
                tr3(u).wait_send()
            hb(u).wait_send()

        return carry

    lax.fori_loop(0, T, drain, 0)

    for i in range(NP):
        @pl.when(home)
        def _():
            hl_copy(i).wait_send()

        @pl.when(peer)
        def _():
            xl_copy(i).wait_send()

    for k in range(FC):
        cols = slice(k * fw, (k + 1) * fw)
        f2_copy(k).wait_recv()
        branch = acc[r, :, cols] + xr2[:, cols]
        y_ref[:, cols] = (xv[:, cols].astype(jnp.float32) + branch).astype(jnp.bfloat16)
    for k in range(FC):
        for i in range(2):
            f_copy(i, k).wait_send()
        f2_copy(k).wait_send()


def solution(mesh):
    def local_block(x_blk, gain_blk, w_in_blk, w_out_blk):
        d_loc = x_blk.shape[1]
        kdim, ff_loc = w_in_blk.shape
        w = ff_loc // (2 * T)
        ntok = ROWS * TOK
        f32, bf16 = jnp.float32, jnp.bfloat16
        dma = pltpu.SemaphoreType.DMA
        nd = max(ND, 8)
        scratch = [
            pltpu.VMEM((TOK, d_loc), bf16),
            pltpu.VMEM((1, d_loc), f32),
            pltpu.VMEM((ROWS, TOK, kdim), bf16),
            pltpu.VMEM((2, 2, TOK, kdim // 2), bf16),
            pltpu.VMEM((1, kdim), f32),
            pltpu.VMEM((2 * ROWS, 8, 128), f32),
            pltpu.VMEM((ntok, kdim), bf16),
            pltpu.VMEM((NU, 2, kdim, w), bf16),
            pltpu.VMEM((NDN, w, d_loc), bf16),
            pltpu.VMEM((T, ntok, w), f32),
            pltpu.VMEM((T, ntok, w), f32),
            pltpu.VMEM((T, ntok, w), f32),
            pltpu.VMEM((T, max(NA, NB), w), f32),
            pltpu.VMEM((ntok, w), f32),
            pltpu.VMEM((T, nd, w), f32),
            pltpu.VMEM((T, nd, w), f32),
            pltpu.VMEM((T, nd, w), f32),
            pltpu.VMEM((T, ntok, w), bf16),
            pltpu.VMEM((T, NB, w), bf16),
            pltpu.VMEM((ROWS, TOK, d_loc), f32),
            pltpu.VMEM((2, TOK, d_loc), f32),
            pltpu.VMEM((TOK, d_loc), f32),
            pltpu.VMEM((TOK, d_loc), f32),
            dma((2,)), dma((4, 2)), dma((ROWS, 2)), dma((2, 2)), dma((2, 2)), dma((NP,)), dma((NP,)), dma((NP,)), dma((NP,)), dma, dma, dma((2 * ROWS,)), dma((2 * ROWS,)),
            dma((NU, 2)), dma((NDN,)),
        ] + [dma((T,))] * 18 + [dma((2, FC)), dma((2, FC)), dma((FC,)), dma((FC,))]
        return pl.pallas_call(
            mlp_kernel,
            out_shape=jax.ShapeDtypeStruct((TOK, d_loc), bf16),
            in_specs=[pl.BlockSpec(memory_space=pl.ANY)] * 4,
            out_specs=pl.BlockSpec(memory_space=pltpu.VMEM),
            scratch_shapes=scratch,
            compiler_params=pltpu.CompilerParams(
                collective_id=0, has_side_effects=True, vmem_limit_bytes=67_043_328),
        )(x_blk, gain_blk.reshape(1, d_loc), w_in_blk, w_out_blk)

    return jax.shard_map(
        local_block,
        mesh=mesh,
        in_specs=(P(("dp", "row"), "col"), P("col"), P("row", "col"), P("row", "col")),
        out_specs=P(("dp", "row"), "col"),
        check_vma=False,
    )
```

```python
import functools
import math

import jax
import jax.numpy as jnp
from jax import lax
from jax.experimental import pallas as pl
from jax.experimental.pallas import tpu as pltpu
from jax.sharding import PartitionSpec as P

NORM_EPS = 1e-5
MESH = pl.DeviceIdType.MESH

TOK = 24
ROWS = 4
T = 16
NB = 32
NA = 40
ND = 24
NU = 5
NDN = 5
XRELAY = 3
LA, LB, LG, LF = 3, 5, 7, 8
LH, LP = 8, 10
LX = 4
TN = T - 1
NP = 3
FC = 4


def gelu_tanh(v):
    inner = math.sqrt(2.0 / math.pi) * (v + 0.044715 * (v * v * v))
    return v * (0.5 * (1.0 + jnp.tanh(inner)))


def mlp_kernel(
    x_hbm, g_hbm, wi_hbm, wo_hbm, y_ref,
    xv, gv, xblk, xrel, gblk, stat, z, usl, dsl, p_own, p_oth, r_d2d, xr, xl, t1, t2, t3, h, hs, acc, dr, fs, xr2,
    ld_s, xs_s, xs_r, xo_s, xo_r, l_s, xl_r, hl_r, g_s, g_r, st_s, st_r, u_sem, d_sem,
    d2d_s, d2d_r, x_s, x_r, t_s, t_r, y_s, y_r, b_s, b_r, f_s, f_r, f2_s, f2_r,
):
    r = lax.axis_index("row")
    c = lax.axis_index("col")
    xc = r // 2
    q = r % 2
    home = xc == c
    peer = xc != c
    pair = 2 * xc + (1 - q)
    xrow = 2 * (1 - xc) + q
    ycol = 1 - c
    d_loc = x_hbm.shape[1]
    kdim = z.shape[1]
    w = h.shape[2]
    ntok = ROWS * TOK
    d_model = 2 * d_loc
    half = T * w

    def rcopy(src, dst, ssem, rsem, row, col):
        return pltpu.make_async_remote_copy(
            src_ref=src, dst_ref=dst, send_sem=ssem, recv_sem=rsem,
            device_id={"row": row, "col": col}, device_id_type=MESH)

    ld_x = pltpu.make_async_copy(x_hbm, xv, ld_s.at[0])
    ld_g = pltpu.make_async_copy(g_hbm, gv, ld_s.at[1])
    ld_x.start()
    ld_g.start()

    barrier = pltpu.get_barrier_semaphore()
    for k in range(1, 2 * ROWS):
        rr = lax.rem(r + k, ROWS)
        cc = lax.rem(c + k // ROWS, 2)
        pl.semaphore_signal(barrier, inc=1, device_id={"row": rr, "col": cc}, device_id_type=MESH)

    def u_copy(s, k):
        slot = lax.rem(s, NU)
        side = q if k == 1 else 1 - q
        cols = pl.ds(pl.multiple_of(side * half + s * w, w), w)
        return pltpu.make_async_copy(wi_hbm.at[:, cols], usl.at[slot, k], u_sem.at[slot, k])

    def d_copy(s):
        slot = lax.rem(s, NDN)
        rows = pl.ds(pl.multiple_of(s * w, w), w)
        return pltpu.make_async_copy(wo_hbm.at[rows, :], dsl.at[slot], d_sem.at[slot])

    ld_x.wait()
    ld_g.wait()
    for s in range(NU):
        u_copy(s, 0).start()
        u_copy(s, 1).start()
    for s in range(NDN):
        d_copy(s).start()

    s1 = jnp.zeros((TOK, 128), jnp.float32)
    s2 = jnp.zeros((TOK, 128), jnp.float32)
    for j in range(d_loc // 128):
        v = xv[:, j * 128:(j + 1) * 128].astype(jnp.float32)
        s1 = s1 + v
        s2 = s2 + v * v
    s1 = jnp.sum(s1, axis=1, keepdims=True)
    s2 = jnp.sum(s2, axis=1, keepdims=True)
    lane = lax.broadcasted_iota(jnp.int32, (8, 128), 1)
    me = c * ROWS + r
    st = jnp.zeros((8, 128), jnp.float32)
    for i in range(TOK // 8):
        st = jnp.where(lane == 2 * i, s1[8 * i:8 * i + 8], st)
        st = jnp.where(lane == 2 * i + 1, s2[8 * i:8 * i + 8], st)
    stat[me] = st

    @pl.when(home)
    def _():
        gblk[...] = gv[:, pl.ds(pl.multiple_of(q * kdim, kdim), kdim)]
        for j in range(2):
            @pl.when(q == j)
            def _():
                xblk[r] = xv[:, j * kdim:(j + 1) * kdim]

    pl.semaphore_wait(barrier, 2 * ROWS - 1)

    def st_copy(k):
        rr = lax.rem(r + k, ROWS)
        cc = lax.rem(c + k // ROWS, 2)
        return rcopy(stat.at[me], stat.at[me], st_s, st_r, rr, cc)

    for k in range(1, 2 * ROWS):
        st_copy(k).start()

    xw = kdim // 2

    def xcols(j, p):
        return pl.ds(j * kdim + p * xw, xw)

    def xs_home_pair(p):
        cols = pl.ds(pl.multiple_of((1 - q) * kdim + p * xw, xw), xw)
        return rcopy(xv.at[:, cols], xblk.at[r, :, pl.ds(p * xw, xw)], xs_s, xs_r, pair, c)

    def xs_home_y(j, p):
        return rcopy(xv.at[:, xcols(j, p)], xblk.at[r, :, pl.ds(p * xw, xw)], xs_s, xs_r,
                     2 * xc + j, ycol)

    def xs_peer_x(j, p):
        return rcopy(xv.at[:, xcols(j, p)], xblk.at[r, :, pl.ds(p * xw, xw)], xs_s, xs_r,
                     2 * (1 - xc) + j, c)

    def xs_peer_far(j, p):
        return rcopy(xv.at[:, xcols(j, p)], xblk.at[r, :, pl.ds(p * xw, xw)], xs_s, xs_r,
                     2 * (1 - xc) + j, ycol)

    def xs_relay_in(j, p):
        return rcopy(xv.at[:, xcols(j, p)], xrel.at[2 * p + j], xs_s, xo_r.at[j, p], r, ycol)

    def xs_relay_out(j, p):
        return rcopy(xrel.at[2 * p + j], xblk.at[r, :, pl.ds(p * xw, xw)], xo_s, xs_r,
                     2 * (1 - xc) + j, c)

    pieces = [(j, p) for p in range(2) for j in range(2)]

    def g_copy():
        return rcopy(gv.at[:, pl.ds(pl.multiple_of(q * kdim, kdim), kdim)], gblk, g_s, g_r, r, ycol)

    @pl.when(home)
    def _():
        for j, p in pieces:
            xs_home_y(j, p).start()
        for p in range(2):
            xs_home_pair(p).start()
        g_copy().start()

    @pl.when(peer)
    def _():
        for n, (j, p) in enumerate(pieces):
            if n < XRELAY:
                xs_relay_in(j, p).start()
            else:
                xs_peer_far(j, p).start()
        for j, p in pieces:
            xs_peer_x(j, p).start()

    acc[...] = jnp.zeros_like(acc)

    @pl.when(home)
    def _():
        for n, (j, p) in enumerate(pieces):
            if n < XRELAY:
                xs_relay_in(j, p).wait_recv()
                xs_relay_out(j, p).start()

    others = stat.at[pl.ds(0, 2 * ROWS - 1)]
    rcopy(others, others, st_s, st_r, r, ycol).wait_recv()

    @pl.when(home)
    def _():
        three = xblk.at[pl.ds(0, ROWS - 1)]
        rcopy(three, three, xs_s, xs_r, r, ycol).wait_recv()

    @pl.when(peer)
    def _():
        rcopy(xblk, xblk, xs_s, xs_r, r, ycol).wait_recv()

    @pl.when(peer)
    def _():
        g_copy().wait_recv()

    means, invs = [], []
    for rr in range(ROWS):
        tot = (stat[rr] + stat[ROWS + rr]) / d_model
        mean = jnp.concatenate([tot[:, 2 * i:2 * i + 1] for i in range(TOK // 8)], axis=0)
        var = jnp.concatenate([tot[:, 2 * i + 1:2 * i + 2] for i in range(TOK // 8)], axis=0) - mean * mean
        means.append(mean)
        invs.append(lax.rsqrt(var + NORM_EPS))
    zw = 512
    for j in range(kdim // zw):
        cols = slice(j * zw, (j + 1) * zw)
        g = gblk[:, cols]
        parts = []
        for rr in range(ROWS):
            v = xblk[rr, :, cols].astype(jnp.float32)
            parts.append((v - means[rr]) * invs[rr] * g)
        z[:, cols] = jnp.concatenate(parts, axis=0).astype(jnp.bfloat16)

    def d2d(u):
        return rcopy(p_oth.at[u], r_d2d.at[u], d2d_s, d2d_r.at[u], pair, c)

    def xa(u):
        return rcopy(p_own.at[u, pl.ds(NB, NA)], xr.at[u, pl.ds(0, NA)], x_s, x_r.at[u], xrow, c)

    prow = ntok // NP

    def xl_copy(i):
        rows = pl.ds(pl.multiple_of(i * prow, prow), prow)
        return rcopy(p_own.at[TN, rows], xl.at[rows], l_s, xl_r.at[i], xrow, c)

    def xb(u):
        return rcopy(p_own.at[u, pl.ds(0, NB)], xr.at[u, pl.ds(0, NB)], x_s, x_r.at[u], xrow, c)

    def tr1(u):
        return rcopy(p_own.at[u, pl.ds(NB + NA, ND)], t1.at[u], t_s, t_r.at[u], r, ycol)

    def tr2(u):
        return rcopy(t1.at[u], t2.at[u], t_s, t_r.at[u], xrow, c)

    def tr3(u):
        return rcopy(t2.at[u], t3.at[u], y_s, y_r.at[u], r, ycol)

    def hb(u):
        return rcopy(hs.at[u], h.at[u, pl.ds(0, NB)], b_s, b_r.at[u], xrow, c)

    def hay(u):
        rows = pl.ds(NB, ntok - NB)
        return rcopy(h.at[u, rows], h.at[u, rows], y_s, y_r.at[u], r, ycol)

    def hl_copy(i):
        rows = pl.ds(pl.multiple_of(i * prow, prow), prow)
        return rcopy(h.at[TN, rows], h.at[TN, rows], l_s, hl_r, r, ycol)

    def hby(u):
        rows = pl.ds(0, NB)
        return rcopy(h.at[u, rows], h.at[u, rows], b_s, b_r.at[u], r, ycol)

    def live(v):
        return jnp.logical_and(v >= 0, v < TN)

    def live_piece(i):
        return jnp.logical_and(i >= 0, i < NP)

    def step(s, carry):
        vg = s - LG

        @pl.when(jnp.logical_and(live(vg), home))
        def _():
            xa(vg).wait_recv()
            got = xr[vg, 0:NA]
            if ND:
                tr3(vg).wait_recv()
                got = jnp.concatenate([got, t3[vg]], axis=0)
            h[vg, NB:ntok] = gelu_tanh(p_own[vg, NB:ntok] + got).astype(jnp.bfloat16)

        @pl.when(jnp.logical_and(live(vg), peer))
        def _():
            xb(vg).wait_recv()
            hs[vg] = gelu_tanh(p_own[vg, 0:NB] + xr[vg, 0:NB]).astype(jnp.bfloat16)

        ig = s - T - LX

        @pl.when(jnp.logical_and(live_piece(ig), home))
        def _():
            xl_copy(ig).wait_recv()
            rows = pl.ds(pl.multiple_of(ig * prow, prow), prow)
            h[TN, rows] = gelu_tanh(p_own[TN, rows] + xl[rows]).astype(jnp.bfloat16)

        slot = lax.rem(s, NU)

        @pl.when(s < T)
        def _():
            u_copy(s, 0).wait()
            p_oth[s] = jnp.dot(z[...], usl[slot, 0], preferred_element_type=jnp.float32)

        @pl.when(jnp.logical_and(live(vg), home))
        def _():
            hay(vg).start()

        @pl.when(jnp.logical_and(live_piece(ig), home))
        def _():
            hl_copy(ig).start()

        @pl.when(jnp.logical_and(live(vg), peer))
        def _():
            hb(vg).start()

        if ND:
            va = s - LA

            @pl.when(jnp.logical_and(live(va), home))
            def _():
                tr1(va).wait_recv()
                tr2(va).start()

            vb = s - LB

            @pl.when(jnp.logical_and(live(vb), peer))
            def _():
                tr2(vb).wait_recv()
                tr3(vb).start()

        u = s - 1

        @pl.when(jnp.logical_and(u >= 0, u < T))
        def _():
            d2d(u).wait_recv()
            p_own[u] = p_own[u] + r_d2d[u]

        @pl.when(s < T)
        def _():
            d2d(s).start()

        @pl.when(jnp.logical_and(live(u), home))
        def _():
            xb(u).start()

        @pl.when(jnp.logical_and(live(u), peer))
        def _():
            if ND:
                tr1(u).start()
            xa(u).start()

        @pl.when(jnp.logical_and(live_piece(s - T), peer))
        def _():
            xl_copy(s - T).start()

        @pl.when(s < T)
        def _():
            u_copy(s, 1).wait()
            p_own[s] = jnp.dot(z[...], usl[slot, 1], preferred_element_type=jnp.float32)

        @pl.when(s + NU < T)
        def _():
            u_copy(s + NU, 0).start()
            u_copy(s + NU, 1).start()

        vf = s - LF

        @pl.when(jnp.logical_and(live(vf), home))
        def _():
            hb(vf).wait_recv()
            hby(vf).start()

        vd = s - jnp.where(home, LH, LP)

        @pl.when(jnp.logical_and(vd >= 0, vd < T))
        def _():
            @pl.when(jnp.logical_and(live(vd), peer))
            def _():
                hay(vd).wait_recv()
                hby(vd).wait_recv()

            @pl.when(jnp.logical_and(vd == TN, peer))
            def _():
                rcopy(h.at[TN], h.at[TN], l_s, hl_r, r, ycol).wait_recv()

            d_copy(vd).wait()
            dslot = lax.rem(vd, NDN)
            hv = h[vd]
            nw = 512
            for n in range(d_loc // nw):
                cols = slice(n * nw, (n + 1) * nw)
                out = jnp.dot(hv, dsl[dslot, :, cols], preferred_element_type=jnp.float32)
                acc[:, :, cols] = acc[:, :, cols] + out.reshape(ROWS, TOK, nw)

            @pl.when(vd + NDN < T)
            def _():
                d_copy(vd + NDN).start()

        return carry

    lax.fori_loop(0, T + LP, step, 0)

    fw = d_loc // FC
    mine_far = 2 * (1 - xc) + q
    pair_far = 2 * (1 - xc) + (1 - q)

    def fcols(k):
        return pl.ds(k * fw, fw)

    def f_copy(i, k):
        tok = pair_far if i == 0 else pair
        return rcopy(acc.at[tok, :, fcols(k)], dr.at[i, :, fcols(k)], f_s, f_r.at[i, k], pair, c)

    def f2_copy(k):
        return rcopy(fs.at[:, fcols(k)], xr2.at[:, fcols(k)], f2_s, f2_r.at[k], xrow, c)

    for i in range(2):
        for k in range(FC):
            f_copy(i, k).start()
    for k in range(FC):
        cols = slice(k * fw, (k + 1) * fw)
        f_copy(0, k).wait_recv()
        fs[:, cols] = acc[mine_far, :, cols] + dr[0, :, cols]
        if k:
            f2_copy(k - 1).start()
    for k in range(FC):
        cols = slice(k * fw, (k + 1) * fw)
        f_copy(1, k).wait_recv()
        acc[r, :, cols] = acc[r, :, cols] + dr[1, :, cols]
        if k == 0:
            f2_copy(FC - 1).start()

    def all_sent(ref, sem):
        rcopy(ref, ref, sem, d2d_r.at[0], pair, c).wait_send()

    allc = pl.ds(0, TN)
    all_sent(p_oth, d2d_s)
    all_sent(others, st_s)

    @pl.when(home)
    def _():
        all_sent(xblk.at[pl.ds(0, ROWS - 1)], xs_s)
        all_sent(xrel.at[pl.ds(0, XRELAY)], xo_s)
        g_copy().wait_send()
        all_sent(h.at[TN], l_s)
        all_sent(p_own.at[allc, pl.ds(0, NB)], x_s)
        all_sent(h.at[allc, pl.ds(NB, ntok - NB)], y_s)

    @pl.when(peer)
    def _():
        all_sent(xblk, xs_s)
        all_sent(p_own.at[TN], l_s)
        all_sent(p_own.at[allc, pl.ds(NB, NA)], x_s)
        all_sent(t3.at[allc], y_s)

    all_sent(t1.at[allc], t_s)
    all_sent(h.at[allc, pl.ds(0, NB)], b_s)

    for k in range(FC):
        cols = slice(k * fw, (k + 1) * fw)
        f2_copy(k).wait_recv()
        branch = acc[r, :, cols] + xr2[:, cols]
        y_ref[:, cols] = (xv[:, cols].astype(jnp.float32) + branch).astype(jnp.bfloat16)
    all_sent(dr, f_s)
    all_sent(fs, f2_s)


def solution(mesh):
    def local_block(x_blk, gain_blk, w_in_blk, w_out_blk):
        d_loc = x_blk.shape[1]
        kdim, ff_loc = w_in_blk.shape
        w = ff_loc // (2 * T)
        ntok = ROWS * TOK
        f32, bf16 = jnp.float32, jnp.bfloat16
        dma = pltpu.SemaphoreType.DMA
        nd = max(ND, 8)
        scratch = [
            pltpu.VMEM((TOK, d_loc), bf16),
            pltpu.VMEM((1, d_loc), f32),
            pltpu.VMEM((ROWS, TOK, kdim), bf16),
            pltpu.VMEM((4, TOK, kdim // 2), bf16),
            pltpu.VMEM((1, kdim), f32),
            pltpu.VMEM((2 * ROWS, 8, 128), f32),
            pltpu.VMEM((ntok, kdim), bf16),
            pltpu.VMEM((NU, 2, kdim, w), bf16),
            pltpu.VMEM((NDN, w, d_loc), bf16),
            pltpu.VMEM((T, ntok, w), f32),
            pltpu.VMEM((T, ntok, w), f32),
            pltpu.VMEM((T, ntok, w), f32),
            pltpu.VMEM((T, max(NA, NB), w), f32),
            pltpu.VMEM((ntok, w), f32),
            pltpu.VMEM((T, nd, w), f32),
            pltpu.VMEM((T, nd, w), f32),
            pltpu.VMEM((T, nd, w), f32),
            pltpu.VMEM((T, ntok, w), bf16),
            pltpu.VMEM((T, NB, w), bf16),
            pltpu.VMEM((ROWS, TOK, d_loc), f32),
            pltpu.VMEM((2, TOK, d_loc), f32),
            pltpu.VMEM((TOK, d_loc), f32),
            pltpu.VMEM((TOK, d_loc), f32),
            dma((2,)), dma, dma, dma, dma((2, 2)), dma, dma((NP,)), dma, dma, dma, dma, dma,
            dma((NU, 2)), dma((NDN,)),
        ] + [dma, dma((T,))] + [dma, dma((TN,))] * 4 + [dma, dma((2, FC)), dma, dma((FC,))]
        return pl.pallas_call(
            mlp_kernel,
            out_shape=jax.ShapeDtypeStruct((TOK, d_loc), bf16),
            in_specs=[pl.BlockSpec(memory_space=pl.ANY)] * 4,
            out_specs=pl.BlockSpec(memory_space=pltpu.VMEM),
            scratch_shapes=scratch,
            compiler_params=pltpu.CompilerParams(
                collective_id=0, has_side_effects=True, vmem_limit_bytes=67_043_328),
        )(x_blk, gain_blk.reshape(1, d_loc), w_in_blk, w_out_blk)

    return jax.shard_map(
        local_block,
        mesh=mesh,
        in_specs=(P(("dp", "row"), "col"), P("col"), P("row", "col"), P("row", "col")),
        out_specs=P(("dp", "row"), "col"),
        check_vma=False,
    )
```

```python
import functools
import math

import jax
import jax.numpy as jnp
from jax import lax
from jax.experimental import pallas as pl
from jax.experimental.pallas import tpu as pltpu
from jax.sharding import PartitionSpec as P

NORM_EPS = 1e-5
MESH = pl.DeviceIdType.MESH

TOK = 24
ROWS = 4
T = 16
NB = 32
NA = 40
ND = 24
NU = 5
NDN = 5
XRELAY = 3
LA, LB, LG, LF = 3, 5, 7, 8
LH, LP = 9, 10
LX = 6
TN = T - 1
NP = 3
FC = 2


def gelu_tanh(v):
    inner = math.sqrt(2.0 / math.pi) * (v + 0.044715 * (v * v * v))
    return v * (0.5 * (1.0 + jnp.tanh(inner)))


def mlp_kernel(
    x_hbm, g_hbm, wi_hbm, wo_hbm, y_ref,
    xv, gv, xblk, xrel, gblk, stat, z, usl, dsl, p_own, p_oth, r_d2d, xr, xl, t1, t2, t3, h, hs, acc, dr, fs, xr2,
    ld_s, xs_s, xs_r, xo_s, xo_r, l_s, xl_r, hl_r, g_s, g_r, st_s, st_r, u_sem, d_sem,
    d2d_s, d2d_r, x_s, x_r, t_s, t_r, y_s, y_r, b_s, b_r, f_s, f_r, f2_s, f2_r,
):
    r = lax.axis_index("row")
    c = lax.axis_index("col")
    xc = r // 2
    q = r % 2
    home = xc == c
    peer = xc != c
    pair = 2 * xc + (1 - q)
    xrow = 2 * (1 - xc) + q
    ycol = 1 - c
    d_loc = x_hbm.shape[1]
    kdim = z.shape[1]
    w = h.shape[2]
    ntok = ROWS * TOK
    d_model = 2 * d_loc
    half = T * w

    def rcopy(src, dst, ssem, rsem, row, col):
        return pltpu.make_async_remote_copy(
            src_ref=src, dst_ref=dst, send_sem=ssem, recv_sem=rsem,
            device_id={"row": row, "col": col}, device_id_type=MESH)

    ld_x = pltpu.make_async_copy(x_hbm, xv, ld_s.at[0])
    ld_g = pltpu.make_async_copy(g_hbm, gv, ld_s.at[1])
    ld_x.start()
    ld_g.start()

    barrier = pltpu.get_barrier_semaphore()
    for k in range(1, 2 * ROWS):
        rr = lax.rem(r + k, ROWS)
        cc = lax.rem(c + k // ROWS, 2)
        pl.semaphore_signal(barrier, inc=1, device_id={"row": rr, "col": cc}, device_id_type=MESH)

    def u_copy(s, k):
        slot = lax.rem(s, NU)
        side = q if k == 1 else 1 - q
        cols = pl.ds(pl.multiple_of(side * half + s * w, w), w)
        return pltpu.make_async_copy(wi_hbm.at[:, cols], usl.at[slot, k], u_sem.at[slot, k])

    def d_copy(s):
        slot = lax.rem(s, NDN)
        rows = pl.ds(pl.multiple_of(s * w, w), w)
        return pltpu.make_async_copy(wo_hbm.at[rows, :], dsl.at[slot], d_sem.at[slot])

    ld_x.wait()
    ld_g.wait()
    for s in range(NU):
        u_copy(s, 0).start()
        u_copy(s, 1).start()
    for s in range(NDN):
        d_copy(s).start()

    s1 = jnp.zeros((TOK, 128), jnp.float32)
    s2 = jnp.zeros((TOK, 128), jnp.float32)
    for j in range(d_loc // 128):
        v = xv[:, j * 128:(j + 1) * 128].astype(jnp.float32)
        s1 = s1 + v
        s2 = s2 + v * v
    s1 = jnp.sum(s1, axis=1, keepdims=True)
    s2 = jnp.sum(s2, axis=1, keepdims=True)
    lane = lax.broadcasted_iota(jnp.int32, (8, 128), 1)
    me = c * ROWS + r
    st = jnp.zeros((8, 128), jnp.float32)
    for i in range(TOK // 8):
        st = jnp.where(lane == 2 * i, s1[8 * i:8 * i + 8], st)
        st = jnp.where(lane == 2 * i + 1, s2[8 * i:8 * i + 8], st)
    stat[me] = st

    @pl.when(home)
    def _():
        gblk[...] = gv[:, pl.ds(pl.multiple_of(q * kdim, kdim), kdim)]
        for j in range(2):
            @pl.when(q == j)
            def _():
                xblk[r] = xv[:, j * kdim:(j + 1) * kdim]

    pl.semaphore_wait(barrier, 2 * ROWS - 1)

    def st_copy(k):
        rr = lax.rem(r + k, ROWS)
        cc = lax.rem(c + k // ROWS, 2)
        return rcopy(stat.at[me], stat.at[me], st_s, st_r, rr, cc)

    for k in range(1, 2 * ROWS):
        st_copy(k).start()

    xw = kdim // 2

    def xcols(j, p):
        return pl.ds(j * kdim + p * xw, xw)

    def xs_home_pair(p):
        cols = pl.ds(pl.multiple_of((1 - q) * kdim + p * xw, xw), xw)
        return rcopy(xv.at[:, cols], xblk.at[r, :, pl.ds(p * xw, xw)], xs_s, xs_r, pair, c)

    def xs_home_y(j, p):
        return rcopy(xv.at[:, xcols(j, p)], xblk.at[r, :, pl.ds(p * xw, xw)], xs_s, xs_r,
                     2 * xc + j, ycol)

    def xs_peer_x(j, p):
        return rcopy(xv.at[:, xcols(j, p)], xblk.at[r, :, pl.ds(p * xw, xw)], xs_s, xs_r,
                     2 * (1 - xc) + j, c)

    def xs_peer_far(j, p):
        return rcopy(xv.at[:, xcols(j, p)], xblk.at[r, :, pl.ds(p * xw, xw)], xs_s, xs_r,
                     2 * (1 - xc) + j, ycol)

    def xs_relay_in(j, p):
        return rcopy(xv.at[:, xcols(j, p)], xrel.at[2 * p + j], xs_s, xo_r.at[j, p], r, ycol)

    def xs_relay_out(j, p):
        return rcopy(xrel.at[2 * p + j], xblk.at[r, :, pl.ds(p * xw, xw)], xo_s, xs_r,
                     2 * (1 - xc) + j, c)

    pieces = [(j, p) for p in range(2) for j in range(2)]

    def g_copy():
        return rcopy(gv.at[:, pl.ds(pl.multiple_of(q * kdim, kdim), kdim)], gblk, g_s, g_r, r, ycol)

    @pl.when(home)
    def _():
        for j, p in pieces:
            xs_home_y(j, p).start()
        for p in range(2):
            xs_home_pair(p).start()
        g_copy().start()

    @pl.when(peer)
    def _():
        for n, (j, p) in enumerate(pieces):
            if n < XRELAY:
                xs_relay_in(j, p).start()
            else:
                xs_peer_far(j, p).start()
        for j, p in pieces:
            xs_peer_x(j, p).start()

    acc[...] = jnp.zeros_like(acc)

    @pl.when(home)
    def _():
        for n, (j, p) in enumerate(pieces):
            if n < XRELAY:
                xs_relay_in(j, p).wait_recv()
                xs_relay_out(j, p).start()

    others = stat.at[pl.ds(0, 2 * ROWS - 1)]
    rcopy(others, others, st_s, st_r, r, ycol).wait_recv()

    @pl.when(home)
    def _():
        three = xblk.at[pl.ds(0, ROWS - 1)]
        rcopy(three, three, xs_s, xs_r, r, ycol).wait_recv()

    @pl.when(peer)
    def _():
        rcopy(xblk, xblk, xs_s, xs_r, r, ycol).wait_recv()

    @pl.when(peer)
    def _():
        g_copy().wait_recv()

    means, invs = [], []
    for rr in range(ROWS):
        tot = (stat[rr] + stat[ROWS + rr]) / d_model
        mean = jnp.concatenate([tot[:, 2 * i:2 * i + 1] for i in range(TOK // 8)], axis=0)
        var = jnp.concatenate([tot[:, 2 * i + 1:2 * i + 2] for i in range(TOK // 8)], axis=0) - mean * mean
        means.append(mean)
        invs.append(lax.rsqrt(var + NORM_EPS))
    zw = 512
    for j in range(kdim // zw):
        cols = slice(j * zw, (j + 1) * zw)
        g = gblk[:, cols]
        parts = []
        for rr in range(ROWS):
            v = xblk[rr, :, cols].astype(jnp.float32)
            parts.append((v - means[rr]) * invs[rr] * g)
        z[:, cols] = jnp.concatenate(parts, axis=0).astype(jnp.bfloat16)

    def d2d(u):
        return rcopy(p_oth.at[u], r_d2d.at[u], d2d_s, d2d_r.at[u], pair, c)

    def xa(u):
        return rcopy(p_own.at[u, pl.ds(NB, NA)], xr.at[u, pl.ds(0, NA)], x_s, x_r.at[u], xrow, c)

    prow = ntok // NP

    def xl_copy(i):
        rows = pl.ds(pl.multiple_of(i * prow, prow), prow)
        return rcopy(p_own.at[TN, rows], xl.at[rows], l_s, xl_r.at[i], xrow, c)

    def xb(u):
        return rcopy(p_own.at[u, pl.ds(0, NB)], xr.at[u, pl.ds(0, NB)], x_s, x_r.at[u], xrow, c)

    def tr1(u):
        return rcopy(p_own.at[u, pl.ds(NB + NA, ND)], t1.at[u], t_s, t_r.at[u], r, ycol)

    def tr2(u):
        return rcopy(t1.at[u], t2.at[u], t_s, t_r.at[u], xrow, c)

    def tr3(u):
        return rcopy(t2.at[u], t3.at[u], y_s, y_r.at[u], r, ycol)

    def hb(u):
        return rcopy(hs.at[u], h.at[u, pl.ds(0, NB)], b_s, b_r.at[u], xrow, c)

    def hay(u):
        rows = pl.ds(NB, ntok - NB)
        return rcopy(h.at[u, rows], h.at[u, rows], y_s, y_r.at[u], r, ycol)

    def hl_copy(i):
        rows = pl.ds(pl.multiple_of(i * prow, prow), prow)
        return rcopy(h.at[TN, rows], h.at[TN, rows], l_s, hl_r, r, ycol)

    def hby(u):
        rows = pl.ds(0, NB)
        return rcopy(h.at[u, rows], h.at[u, rows], b_s, b_r.at[u], r, ycol)

    def live(v):
        return jnp.logical_and(v >= 0, v < TN)

    def live_piece(i):
        return jnp.logical_and(i >= 0, i < NP)

    def step(s, carry):
        vg = s - LG

        @pl.when(jnp.logical_and(live(vg), home))
        def _():
            xa(vg).wait_recv()
            got = xr[vg, 0:NA]
            if ND:
                tr3(vg).wait_recv()
                got = jnp.concatenate([got, t3[vg]], axis=0)
            h[vg, NB:ntok] = gelu_tanh(p_own[vg, NB:ntok] + got).astype(jnp.bfloat16)

        @pl.when(jnp.logical_and(live(vg), peer))
        def _():
            xb(vg).wait_recv()
            hs[vg] = gelu_tanh(p_own[vg, 0:NB] + xr[vg, 0:NB]).astype(jnp.bfloat16)

        ig = s - T - LX

        @pl.when(jnp.logical_and(live_piece(ig), home))
        def _():
            xl_copy(ig).wait_recv()
            rows = pl.ds(pl.multiple_of(ig * prow, prow), prow)
            h[TN, rows] = gelu_tanh(p_own[TN, rows] + xl[rows]).astype(jnp.bfloat16)

        slot = lax.rem(s, NU)

        @pl.when(s < T)
        def _():
            u_copy(s, 0).wait()
            p_oth[s] = jnp.dot(z[...], usl[slot, 0], preferred_element_type=jnp.float32)

        @pl.when(jnp.logical_and(live(vg), home))
        def _():
            hay(vg).start()

        @pl.when(jnp.logical_and(live_piece(ig), home))
        def _():
            hl_copy(ig).start()

        @pl.when(jnp.logical_and(live(vg), peer))
        def _():
            hb(vg).start()

        if ND:
            va = s - LA

            @pl.when(jnp.logical_and(live(va), home))
            def _():
                tr1(va).wait_recv()
                tr2(va).start()

            vb = s - LB

            @pl.when(jnp.logical_and(live(vb), peer))
            def _():
                tr2(vb).wait_recv()
                tr3(vb).start()

        u = s - 1

        @pl.when(jnp.logical_and(u >= 0, u < T))
        def _():
            d2d(u).wait_recv()
            p_own[u] = p_own[u] + r_d2d[u]

        @pl.when(s < T)
        def _():
            d2d(s).start()

        @pl.when(jnp.logical_and(live(u), home))
        def _():
            xb(u).start()

        @pl.when(jnp.logical_and(live(u), peer))
        def _():
            if ND:
                tr1(u).start()
            xa(u).start()

        @pl.when(jnp.logical_and(live_piece(s - T), peer))
        def _():
            xl_copy(s - T).start()

        @pl.when(s < T)
        def _():
            u_copy(s, 1).wait()
            p_own[s] = jnp.dot(z[...], usl[slot, 1], preferred_element_type=jnp.float32)

        @pl.when(s + NU < T)
        def _():
            u_copy(s + NU, 0).start()
            u_copy(s + NU, 1).start()

        vf = s - LF

        @pl.when(jnp.logical_and(live(vf), home))
        def _():
            hb(vf).wait_recv()
            hby(vf).start()

        vd = s - jnp.where(home, LH, LP)

        @pl.when(jnp.logical_and(vd >= 0, vd < T))
        def _():
            @pl.when(jnp.logical_and(live(vd), peer))
            def _():
                hay(vd).wait_recv()
                hby(vd).wait_recv()

            @pl.when(jnp.logical_and(vd == TN, peer))
            def _():
                rcopy(h.at[TN], h.at[TN], l_s, hl_r, r, ycol).wait_recv()

            d_copy(vd).wait()
            dslot = lax.rem(vd, NDN)
            hv = h[vd]
            nw = 512
            for n in range(d_loc // nw):
                cols = slice(n * nw, (n + 1) * nw)
                out = jnp.dot(hv, dsl[dslot, :, cols], preferred_element_type=jnp.float32)
                acc[:, :, cols] = acc[:, :, cols] + out.reshape(ROWS, TOK, nw)

            @pl.when(vd + NDN < T)
            def _():
                d_copy(vd + NDN).start()

        return carry

    lax.fori_loop(0, T + LP, step, 0)

    fw = d_loc // FC
    mine_far = 2 * (1 - xc) + q
    pair_far = 2 * (1 - xc) + (1 - q)

    def fcols(k):
        return pl.ds(k * fw, fw)

    def f_copy(i, k):
        tok = pair_far if i == 0 else pair
        return rcopy(acc.at[tok, :, fcols(k)], dr.at[i, :, fcols(k)], f_s, f_r.at[i, k], pair, c)

    def f2_copy(k):
        return rcopy(fs.at[:, fcols(k)], xr2.at[:, fcols(k)], f2_s, f2_r.at[k], xrow, c)

    for i in range(2):
        for k in range(FC):
            f_copy(i, k).start()
    for k in range(FC):
        cols = slice(k * fw, (k + 1) * fw)
        f_copy(0, k).wait_recv()
        fs[:, cols] = acc[mine_far, :, cols] + dr[0, :, cols]
        if k:
            f2_copy(k - 1).start()
    for k in range(FC):
        cols = slice(k * fw, (k + 1) * fw)
        f_copy(1, k).wait_recv()
        acc[r, :, cols] = acc[r, :, cols] + dr[1, :, cols]
        if k == 0:
            f2_copy(FC - 1).start()

    def all_sent(ref, sem):
        rcopy(ref, ref, sem, d2d_r.at[0], pair, c).wait_send()

    allc = pl.ds(0, TN)
    all_sent(p_oth, d2d_s)
    all_sent(others, st_s)

    @pl.when(home)
    def _():
        all_sent(xblk.at[pl.ds(0, ROWS - 1)], xs_s)
        all_sent(xrel.at[pl.ds(0, XRELAY)], xo_s)
        g_copy().wait_send()
        all_sent(h.at[TN], l_s)
        all_sent(p_own.at[allc, pl.ds(0, NB)], x_s)
        all_sent(h.at[allc, pl.ds(NB, ntok - NB)], y_s)

    @pl.when(peer)
    def _():
        all_sent(xblk, xs_s)
        all_sent(p_own.at[TN], l_s)
        all_sent(p_own.at[allc, pl.ds(NB, NA)], x_s)
        all_sent(t3.at[allc], y_s)

    all_sent(t1.at[allc], t_s)
    all_sent(h.at[allc, pl.ds(0, NB)], b_s)

    for k in range(FC):
        cols = slice(k * fw, (k + 1) * fw)
        f2_copy(k).wait_recv()
        branch = acc[r, :, cols] + xr2[:, cols]
        y_ref[:, cols] = (xv[:, cols].astype(jnp.float32) + branch).astype(jnp.bfloat16)
    all_sent(dr, f_s)
    all_sent(fs, f2_s)


def solution(mesh):
    def local_block(x_blk, gain_blk, w_in_blk, w_out_blk):
        d_loc = x_blk.shape[1]
        kdim, ff_loc = w_in_blk.shape
        w = ff_loc // (2 * T)
        ntok = ROWS * TOK
        f32, bf16 = jnp.float32, jnp.bfloat16
        dma = pltpu.SemaphoreType.DMA
        nd = max(ND, 8)
        scratch = [
            pltpu.VMEM((TOK, d_loc), bf16),
            pltpu.VMEM((1, d_loc), f32),
            pltpu.VMEM((ROWS, TOK, kdim), bf16),
            pltpu.VMEM((4, TOK, kdim // 2), bf16),
            pltpu.VMEM((1, kdim), f32),
            pltpu.VMEM((2 * ROWS, 8, 128), f32),
            pltpu.VMEM((ntok, kdim), bf16),
            pltpu.VMEM((NU, 2, kdim, w), bf16),
            pltpu.VMEM((NDN, w, d_loc), bf16),
            pltpu.VMEM((T, ntok, w), f32),
            pltpu.VMEM((T, ntok, w), f32),
            pltpu.VMEM((T, ntok, w), f32),
            pltpu.VMEM((T, max(NA, NB), w), f32),
            pltpu.VMEM((ntok, w), f32),
            pltpu.VMEM((T, nd, w), f32),
            pltpu.VMEM((T, nd, w), f32),
            pltpu.VMEM((T, nd, w), f32),
            pltpu.VMEM((T, ntok, w), bf16),
            pltpu.VMEM((T, NB, w), bf16),
            pltpu.VMEM((ROWS, TOK, d_loc), f32),
            pltpu.VMEM((2, TOK, d_loc), f32),
            pltpu.VMEM((TOK, d_loc), f32),
            pltpu.VMEM((TOK, d_loc), f32),
        ]
        semaphores = [
            dma((2,)), dma, dma, dma, dma((2, 2)), dma, dma((NP,)), dma, dma, dma, dma, dma,
            dma((NU, 2)), dma((NDN,)),
        ] + [dma, dma((T,))] + [dma, dma((TN,))] * 4 + [dma, dma((2, FC)), dma, dma((FC,))]

        def scoped_kernel(*refs):
            pl.run_scoped(lambda *sems: mlp_kernel(*refs, *sems), *semaphores)

        return pl.pallas_call(
            scoped_kernel,
            out_shape=jax.ShapeDtypeStruct((TOK, d_loc), bf16),
            in_specs=[pl.BlockSpec(memory_space=pl.ANY)] * 4,
            out_specs=pl.BlockSpec(memory_space=pltpu.VMEM),
            scratch_shapes=scratch,
            compiler_params=pltpu.CompilerParams(
                collective_id=0, has_side_effects=True, vmem_limit_bytes=67_043_328),
        )(x_blk, gain_blk.reshape(1, d_loc), w_in_blk, w_out_blk)

    return jax.shard_map(
        local_block,
        mesh=mesh,
        in_specs=(P(("dp", "row"), "col"), P("col"), P("row", "col"), P("row", "col")),
        out_specs=P(("dp", "row"), "col"),
        check_vma=False,
    )
```

```python
import functools
import math

import jax
import jax.numpy as jnp
from jax import lax
from jax.experimental import pallas as pl
from jax.experimental.pallas import tpu as pltpu
from jax.sharding import PartitionSpec as P

NORM_EPS = 1e-5
MESH = pl.DeviceIdType.MESH

TOK = 24
ROWS = 4
T = 16
NB = 32
NA = 40
ND = 24
NU = 5
NDN = 5
XRELAY = 3
LA, LB, LG, LF = 4, 6, 7, 8
LH, LP = 9, 10
LX = 6
TN = T - 1
NP = 3
FC = 2


def gelu_tanh(v):
    inner = math.sqrt(2.0 / math.pi) * (v + 0.044715 * (v * v * v))
    return v * (0.5 * (1.0 + jnp.tanh(inner)))


def mlp_kernel(
    x_hbm, g_hbm, wi_hbm, wo_hbm, y_ref,
    xv, gv, xblk, xrel, gblk, stat, z, usl, dsl, p_own, p_oth, r_d2d, xr, xl, t1, t2, t3, h, hs, acc, dr, fs, xr2,
    ld_s, xs_s, xs_r, xo_s, xo_r, l_s, xl_r, hl_r, g_s, g_r, st_s, st_r, u_sem, d_sem,
    d2d_s, d2d_r, x_s, x_r, t_s, t_r, y_s, y_r, b_s, b_r, f_s, f_r, f2_s, f2_r,
):
    r = lax.axis_index("row")
    c = lax.axis_index("col")
    xc = r // 2
    q = r % 2
    home = xc == c
    peer = xc != c
    pair = 2 * xc + (1 - q)
    xrow = 2 * (1 - xc) + q
    ycol = 1 - c
    d_loc = x_hbm.shape[1]
    kdim = z.shape[1]
    w = h.shape[2]
    ntok = ROWS * TOK
    d_model = 2 * d_loc
    half = T * w

    def rcopy(src, dst, ssem, rsem, row, col):
        return pltpu.make_async_remote_copy(
            src_ref=src, dst_ref=dst, send_sem=ssem, recv_sem=rsem,
            device_id={"row": row, "col": col}, device_id_type=MESH)

    ld_x = pltpu.make_async_copy(x_hbm, xv, ld_s.at[0])
    ld_g = pltpu.make_async_copy(g_hbm, gv, ld_s.at[1])
    ld_x.start()
    ld_g.start()

    barrier = pltpu.get_barrier_semaphore()
    for k in range(1, 2 * ROWS):
        rr = lax.rem(r + k, ROWS)
        cc = lax.rem(c + k // ROWS, 2)
        pl.semaphore_signal(barrier, inc=1, device_id={"row": rr, "col": cc}, device_id_type=MESH)

    def u_copy(s, k):
        slot = lax.rem(s, NU)
        side = q if k == 1 else 1 - q
        cols = pl.ds(pl.multiple_of(side * half + s * w, w), w)
        return pltpu.make_async_copy(wi_hbm.at[:, cols], usl.at[slot, k], u_sem.at[slot, k])

    def d_copy(s):
        slot = lax.rem(s, NDN)
        rows = pl.ds(pl.multiple_of(s * w, w), w)
        return pltpu.make_async_copy(wo_hbm.at[rows, :], dsl.at[slot], d_sem.at[slot])

    ld_x.wait()
    ld_g.wait()
    for s in range(NU):
        u_copy(s, 0).start()
        u_copy(s, 1).start()
    for s in range(NDN):
        d_copy(s).start()

    s1 = jnp.zeros((TOK, 128), jnp.float32)
    s2 = jnp.zeros((TOK, 128), jnp.float32)
    for j in range(d_loc // 128):
        v = xv[:, j * 128:(j + 1) * 128].astype(jnp.float32)
        s1 = s1 + v
        s2 = s2 + v * v
    s1 = jnp.sum(s1, axis=1, keepdims=True)
    s2 = jnp.sum(s2, axis=1, keepdims=True)
    lane = lax.broadcasted_iota(jnp.int32, (8, 128), 1)
    me = c * ROWS + r
    st = jnp.zeros((8, 128), jnp.float32)
    for i in range(TOK // 8):
        st = jnp.where(lane == 2 * i, s1[8 * i:8 * i + 8], st)
        st = jnp.where(lane == 2 * i + 1, s2[8 * i:8 * i + 8], st)
    stat[me] = st

    @pl.when(home)
    def _():
        gblk[...] = gv[:, pl.ds(pl.multiple_of(q * kdim, kdim), kdim)]
        for j in range(2):
            @pl.when(q == j)
            def _():
                xblk[r] = xv[:, j * kdim:(j + 1) * kdim]

    pl.semaphore_wait(barrier, 2 * ROWS - 1)

    def st_copy(k):
        rr = lax.rem(r + k, ROWS)
        cc = lax.rem(c + k // ROWS, 2)
        return rcopy(stat.at[me], stat.at[me], st_s, st_r, rr, cc)

    for k in range(1, 2 * ROWS):
        st_copy(k).start()

    xw = kdim // 2

    def xcols(j, p):
        return pl.ds(j * kdim + p * xw, xw)

    def xs_home_pair(p):
        cols = pl.ds(pl.multiple_of((1 - q) * kdim + p * xw, xw), xw)
        return rcopy(xv.at[:, cols], xblk.at[r, :, pl.ds(p * xw, xw)], xs_s, xs_r, pair, c)

    def xs_home_y(j, p):
        return rcopy(xv.at[:, xcols(j, p)], xblk.at[r, :, pl.ds(p * xw, xw)], xs_s, xs_r,
                     2 * xc + j, ycol)

    def xs_peer_x(j, p):
        return rcopy(xv.at[:, xcols(j, p)], xblk.at[r, :, pl.ds(p * xw, xw)], xs_s, xs_r,
                     2 * (1 - xc) + j, c)

    def xs_peer_far(j, p):
        return rcopy(xv.at[:, xcols(j, p)], xblk.at[r, :, pl.ds(p * xw, xw)], xs_s, xs_r,
                     2 * (1 - xc) + j, ycol)

    def xs_relay_in(j, p):
        return rcopy(xv.at[:, xcols(j, p)], xrel.at[2 * p + j], xs_s, xo_r.at[j, p], r, ycol)

    def xs_relay_out(j, p):
        return rcopy(xrel.at[2 * p + j], xblk.at[r, :, pl.ds(p * xw, xw)], xo_s, xs_r,
                     2 * (1 - xc) + j, c)

    pieces = [(j, p) for p in range(2) for j in range(2)]

    def g_copy():
        return rcopy(gv.at[:, pl.ds(pl.multiple_of(q * kdim, kdim), kdim)], gblk, g_s, g_r, r, ycol)

    @pl.when(home)
    def _():
        for j, p in pieces:
            xs_home_y(j, p).start()
        for p in range(2):
            xs_home_pair(p).start()
        g_copy().start()

    @pl.when(peer)
    def _():
        for n, (j, p) in enumerate(pieces):
            if n < XRELAY:
                xs_relay_in(j, p).start()
            else:
                xs_peer_far(j, p).start()
        for j, p in pieces:
            xs_peer_x(j, p).start()

    acc[...] = jnp.zeros_like(acc)

    @pl.when(home)
    def _():
        for n, (j, p) in enumerate(pieces):
            if n < XRELAY:
                xs_relay_in(j, p).wait_recv()
                xs_relay_out(j, p).start()

    others = stat.at[pl.ds(0, 2 * ROWS - 1)]
    rcopy(others, others, st_s, st_r, r, ycol).wait_recv()

    @pl.when(home)
    def _():
        three = xblk.at[pl.ds(0, ROWS - 1)]
        rcopy(three, three, xs_s, xs_r, r, ycol).wait_recv()

    @pl.when(peer)
    def _():
        rcopy(xblk, xblk, xs_s, xs_r, r, ycol).wait_recv()

    @pl.when(peer)
    def _():
        g_copy().wait_recv()

    means, invs = [], []
    for rr in range(ROWS):
        tot = (stat[rr] + stat[ROWS + rr]) / d_model
        mean = jnp.concatenate([tot[:, 2 * i:2 * i + 1] for i in range(TOK // 8)], axis=0)
        var = jnp.concatenate([tot[:, 2 * i + 1:2 * i + 2] for i in range(TOK // 8)], axis=0) - mean * mean
        means.append(mean)
        invs.append(lax.rsqrt(var + NORM_EPS))
    zw = 512
    for j in range(kdim // zw):
        cols = slice(j * zw, (j + 1) * zw)
        g = gblk[:, cols]
        parts = []
        for rr in range(ROWS):
            v = xblk[rr, :, cols].astype(jnp.float32)
            parts.append((v - means[rr]) * invs[rr] * g)
        z[:, cols] = jnp.concatenate(parts, axis=0).astype(jnp.bfloat16)

    def d2d(u):
        return rcopy(p_oth.at[u], r_d2d.at[u], d2d_s, d2d_r.at[u], pair, c)

    def xa(u):
        return rcopy(p_own.at[u, pl.ds(NB, NA)], xr.at[u, pl.ds(0, NA)], x_s, x_r.at[u], xrow, c)

    prow = ntok // NP

    def xl_copy(i):
        rows = pl.ds(pl.multiple_of(i * prow, prow), prow)
        return rcopy(p_own.at[TN, rows], xl.at[rows], l_s, xl_r.at[i], xrow, c)

    def xb(u):
        return rcopy(p_own.at[u, pl.ds(0, NB)], xr.at[u, pl.ds(0, NB)], x_s, x_r.at[u], xrow, c)

    def tr1(u):
        return rcopy(p_own.at[u, pl.ds(NB + NA, ND)], t1.at[u], t_s, t_r.at[u], r, ycol)

    def tr2(u):
        return rcopy(t1.at[u], t2.at[u], t_s, t_r.at[u], xrow, c)

    def tr3(u):
        return rcopy(t2.at[u], t3.at[u], y_s, y_r.at[u], r, ycol)

    def hb(u):
        return rcopy(hs.at[u], h.at[u, pl.ds(0, NB)], b_s, b_r.at[u], xrow, c)

    def hay(u):
        rows = pl.ds(NB, ntok - NB)
        return rcopy(h.at[u, rows], h.at[u, rows], y_s, y_r.at[u], r, ycol)

    def hl_copy(i):
        rows = pl.ds(pl.multiple_of(i * prow, prow), prow)
        return rcopy(h.at[TN, rows], h.at[TN, rows], l_s, hl_r, r, ycol)

    def hby(u):
        rows = pl.ds(0, NB)
        return rcopy(h.at[u, rows], h.at[u, rows], b_s, b_r.at[u], r, ycol)

    def live(v):
        return jnp.logical_and(v >= 0, v < TN)

    def live_piece(i):
        return jnp.logical_and(i >= 0, i < NP)

    def step(s, carry):
        vg = s - LG

        @pl.when(jnp.logical_and(live(vg), home))
        def _():
            xa(vg).wait_recv()
            got = xr[vg, 0:NA]
            if ND:
                tr3(vg).wait_recv()
                got = jnp.concatenate([got, t3[vg]], axis=0)
            h[vg, NB:ntok] = gelu_tanh(p_own[vg, NB:ntok] + got).astype(jnp.bfloat16)

        @pl.when(jnp.logical_and(live(vg), peer))
        def _():
            xb(vg).wait_recv()
            hs[vg] = gelu_tanh(p_own[vg, 0:NB] + xr[vg, 0:NB]).astype(jnp.bfloat16)

        ig = s - T - LX

        @pl.when(jnp.logical_and(live_piece(ig), home))
        def _():
            xl_copy(ig).wait_recv()
            rows = pl.ds(pl.multiple_of(ig * prow, prow), prow)
            h[TN, rows] = gelu_tanh(p_own[TN, rows] + xl[rows]).astype(jnp.bfloat16)

        slot = lax.rem(s, NU)

        @pl.when(s < T)
        def _():
            u_copy(s, 0).wait()
            p_oth[s] = jnp.dot(z[...], usl[slot, 0], preferred_element_type=jnp.float32)

        @pl.when(jnp.logical_and(live(vg), home))
        def _():
            hay(vg).start()

        @pl.when(jnp.logical_and(live_piece(ig), home))
        def _():
            hl_copy(ig).start()

        @pl.when(jnp.logical_and(live(vg), peer))
        def _():
            hb(vg).start()

        if ND:
            va = s - LA

            @pl.when(jnp.logical_and(live(va), home))
            def _():
                tr1(va).wait_recv()
                tr2(va).start()

            vb = s - LB

            @pl.when(jnp.logical_and(live(vb), peer))
            def _():
                tr2(vb).wait_recv()
                tr3(vb).start()

        u = s - 1

        @pl.when(jnp.logical_and(u >= 0, u < T))
        def _():
            d2d(u).wait_recv()
            p_own[u] = p_own[u] + r_d2d[u]

        @pl.when(s < T)
        def _():
            d2d(s).start()

        @pl.when(jnp.logical_and(live(u), home))
        def _():
            xb(u).start()

        @pl.when(jnp.logical_and(live(u), peer))
        def _():
            if ND:
                tr1(u).start()
            xa(u).start()

        @pl.when(jnp.logical_and(live_piece(s - T), peer))
        def _():
            xl_copy(s - T).start()

        @pl.when(s < T)
        def _():
            u_copy(s, 1).wait()
            p_own[s] = jnp.dot(z[...], usl[slot, 1], preferred_element_type=jnp.float32)

        @pl.when(s + NU < T)
        def _():
            u_copy(s + NU, 0).start()
            u_copy(s + NU, 1).start()

        vd = s - jnp.where(home, LH, LP)

        @pl.when(jnp.logical_and(vd >= 0, vd < T))
        def _():
            @pl.when(jnp.logical_and(live(vd), peer))
            def _():
                hay(vd).wait_recv()
                hby(vd).wait_recv()

            @pl.when(jnp.logical_and(vd == TN, peer))
            def _():
                rcopy(h.at[TN], h.at[TN], l_s, hl_r, r, ycol).wait_recv()

            d_copy(vd).wait()
            dslot = lax.rem(vd, NDN)
            hv = h[vd]
            nw = 512
            for n in range(d_loc // nw):
                cols = slice(n * nw, (n + 1) * nw)
                out = jnp.dot(hv, dsl[dslot, :, cols], preferred_element_type=jnp.float32)
                acc[:, :, cols] = acc[:, :, cols] + out.reshape(ROWS, TOK, nw)

            @pl.when(vd + NDN < T)
            def _():
                d_copy(vd + NDN).start()

        vf = s - LF

        @pl.when(jnp.logical_and(live(vf), home))
        def _():
            hb(vf).wait_recv()
            hby(vf).start()

        return carry

    lax.fori_loop(0, T + LP, step, 0)

    fw = d_loc // FC
    mine_far = 2 * (1 - xc) + q
    pair_far = 2 * (1 - xc) + (1 - q)

    def fcols(k):
        return pl.ds(k * fw, fw)

    def f_copy(i, k):
        tok = pair_far if i == 0 else pair
        return rcopy(acc.at[tok, :, fcols(k)], dr.at[i, :, fcols(k)], f_s, f_r.at[i, k], pair, c)

    def f2_copy(k):
        return rcopy(fs.at[:, fcols(k)], xr2.at[:, fcols(k)], f2_s, f2_r.at[k], xrow, c)

    for i in range(2):
        for k in range(FC):
            f_copy(i, k).start()
    for k in range(FC):
        cols = slice(k * fw, (k + 1) * fw)
        f_copy(0, k).wait_recv()
        fs[:, cols] = acc[mine_far, :, cols] + dr[0, :, cols]
        if k:
            f2_copy(k - 1).start()
    for k in range(FC):
        cols = slice(k * fw, (k + 1) * fw)
        f_copy(1, k).wait_recv()
        acc[r, :, cols] = acc[r, :, cols] + dr[1, :, cols]
        if k == 0:
            f2_copy(FC - 1).start()

    def all_sent(ref, sem):
        rcopy(ref, ref, sem, d2d_r.at[0], pair, c).wait_send()

    allc = pl.ds(0, TN)
    all_sent(p_oth, d2d_s)
    all_sent(others, st_s)

    @pl.when(home)
    def _():
        all_sent(xblk.at[pl.ds(0, ROWS - 1)], xs_s)
        all_sent(xrel.at[pl.ds(0, XRELAY)], xo_s)
        g_copy().wait_send()
        all_sent(h.at[TN], l_s)
        all_sent(p_own.at[allc, pl.ds(0, NB)], x_s)
        all_sent(h.at[allc, pl.ds(NB, ntok - NB)], y_s)

    @pl.when(peer)
    def _():
        all_sent(xblk, xs_s)
        all_sent(p_own.at[TN], l_s)
        all_sent(p_own.at[allc, pl.ds(NB, NA)], x_s)
        all_sent(t3.at[allc], y_s)

    all_sent(t1.at[allc], t_s)
    all_sent(h.at[allc, pl.ds(0, NB)], b_s)

    for k in range(FC):
        cols = slice(k * fw, (k + 1) * fw)
        f2_copy(k).wait_recv()
        branch = acc[r, :, cols] + xr2[:, cols]
        y_ref[:, cols] = (xv[:, cols].astype(jnp.float32) + branch).astype(jnp.bfloat16)
    all_sent(dr, f_s)
    all_sent(fs, f2_s)


def solution(mesh):
    def local_block(x_blk, gain_blk, w_in_blk, w_out_blk):
        d_loc = x_blk.shape[1]
        kdim, ff_loc = w_in_blk.shape
        w = ff_loc // (2 * T)
        ntok = ROWS * TOK
        f32, bf16 = jnp.float32, jnp.bfloat16
        dma = pltpu.SemaphoreType.DMA
        nd = max(ND, 8)
        scratch = [
            pltpu.VMEM((TOK, d_loc), bf16),
            pltpu.VMEM((1, d_loc), f32),
            pltpu.VMEM((ROWS, TOK, kdim), bf16),
            pltpu.VMEM((4, TOK, kdim // 2), bf16),
            pltpu.VMEM((1, kdim), f32),
            pltpu.VMEM((2 * ROWS, 8, 128), f32),
            pltpu.VMEM((ntok, kdim), bf16),
            pltpu.VMEM((NU, 2, kdim, w), bf16),
            pltpu.VMEM((NDN, w, d_loc), bf16),
            pltpu.VMEM((T, ntok, w), f32),
            pltpu.VMEM((T, ntok, w), f32),
            pltpu.VMEM((T, ntok, w), f32),
            pltpu.VMEM((T, max(NA, NB), w), f32),
            pltpu.VMEM((ntok, w), f32),
            pltpu.VMEM((T, nd, w), f32),
            pltpu.VMEM((T, nd, w), f32),
            pltpu.VMEM((T, nd, w), f32),
            pltpu.VMEM((T, ntok, w), bf16),
            pltpu.VMEM((T, NB, w), bf16),
            pltpu.VMEM((ROWS, TOK, d_loc), f32),
            pltpu.VMEM((2, TOK, d_loc), f32),
            pltpu.VMEM((TOK, d_loc), f32),
            pltpu.VMEM((TOK, d_loc), f32),
        ]
        semaphores = [
            dma((2,)), dma, dma, dma, dma((2, 2)), dma, dma((NP,)), dma, dma, dma, dma, dma,
            dma((NU, 2)), dma((NDN,)),
        ] + [dma, dma((T,))] + [dma, dma((TN,))] * 4 + [dma, dma((2, FC)), dma, dma((FC,))]

        def scoped_kernel(*refs):
            pl.run_scoped(lambda *sems: mlp_kernel(*refs, *sems), *semaphores)

        return pl.pallas_call(
            scoped_kernel,
            out_shape=jax.ShapeDtypeStruct((TOK, d_loc), bf16),
            in_specs=[pl.BlockSpec(memory_space=pl.ANY)] * 4,
            out_specs=pl.BlockSpec(memory_space=pltpu.VMEM),
            scratch_shapes=scratch,
            compiler_params=pltpu.CompilerParams(
                collective_id=0, has_side_effects=True, vmem_limit_bytes=67_043_328),
        )(x_blk, gain_blk.reshape(1, d_loc), w_in_blk, w_out_blk)

    return jax.shard_map(
        local_block,
        mesh=mesh,
        in_specs=(P(("dp", "row"), "col"), P("col"), P("row", "col"), P("row", "col")),
        out_specs=P(("dp", "row"), "col"),
        check_vma=False,
    )
```
